32 devices in a mesh: mp: 8 (over z, y), rows: 4 (over x, core).
Axes of the slice: x: 2, y: 2, z: 4, core: 2. Of those that a mesh axis runs over, the one named last changes fastest.
Arguments:
- inputs: float32 [1024, 16384], P('rows', 'mp'), may hold values from -6 to 6
- weight: float32 [512, 16384], P('mp'), may hold values from -1.5 to 1.5, as said below
Outputs:
- row_scale: float32 [1024], P('rows')
- product: float32 [512, 1024], P('mp', 'rows')
- normalized: float32 [512, 1024], P('mp')
The draws below stay inside these ranges and needn't reach their ends.
Inputs may be any that keep to these rules, and one draw needn't show every extreme that they name: A weight matrix whose rows carry different scales.
All inputs are finite; a program needn't handle non-finite values. Where the reference program divides by a largest or mean magnitude, that divisor is 1e-20 or more.
Results may differ from the reference program's by a relative error of at most 0.0003.
Values may be sent and summed in bfloat16 or wider, within the bound.
A program may use at most 64 MiB of HBM per device.

```python
import math
import jax
import jax.numpy as jnp
from jax import lax

INNER = 16384
COLS_DEV = 64
COLS = 512
ROWS = 1024
N_MP = 8


def draw_weight(key, part):
    base_key, spread_key = jax.random.split(jax.random.fold_in(key, 11))
    columns = jnp.arange(COLS).astype(jnp.float32)
    rising = jnp.sqrt(1.0 + 2.0 * columns / COLS)
    base = jnp.clip(jax.random.normal(base_key, (COLS, INNER), jnp.float32), -6.0, 6.0)
    spread = jnp.exp(jax.random.uniform(spread_key, (COLS,), jnp.float32, 0.0, math.log(10.0)))
    return (base * (spread * rising)[:, None] / 72.0).astype(jnp.float32)


def levels(stream_key, extent, shards, low, top_value):
    level, own = 1.0, jax.random.fold_in(stream_key, 6)
    for axis_at, blocks in shards:
        draws = jnp.exp(jax.random.uniform(jax.random.fold_in(own, axis_at), (blocks,), jnp.float32, low / len(shards), top_value / len(shards)))
        level = level * jnp.repeat(draws, extent[axis_at] // blocks).reshape([-1 if axis == axis_at else 1 for axis in range(len(extent))])
    return level


def scatter_about(rng, shape, width, reach, pieces=(), held_as=jnp.bfloat16):
    level = levels(rng, shape, pieces, -0.22, 0.18) if pieces else 1.0
    entries = jax.random.normal(rng, shape, jnp.float32) * width * level
    return jnp.minimum(jnp.maximum(entries, -reach), reach).astype(held_as)


def setup_inputs(seed: int = 0) -> dict:
    arg_keys = jax.random.split(jax.random.key(seed), 3)
    inputs = scatter_about(arg_keys[0], (ROWS, INNER), 1.0, 6.0, ((0, 4), (1, 8)), jnp.float32)
    weight = draw_weight(jax.random.fold_in(arg_keys[2], 71), 0)
    return dict(inputs=inputs, weight=weight)


epsilon = 1e-06

def split_two(values):
    scaled = values * 128.0
    first = jnp.floor(scaled)
    second = jnp.floor((scaled - first) * 256.0)
    return (first, second)

def reference(inputs, weight):
    row_scale = lax.optimization_barrier(jnp.max(jnp.abs(inputs), axis=1)) + epsilon
    x_parts = split_two(inputs / row_scale[:, None])
    blocks = weight.reshape(N_MP, COLS_DEV, INNER)
    highest = lax.Precision.HIGHEST

    def column_block(w_block):
        col_scale = lax.optimization_barrier(jnp.max(jnp.abs(w_block), axis=1)) + epsilon
        w_parts = split_two(w_block / col_scale[:, None])
        combined = jnp.dot(w_parts[0] + w_parts[1] / 256.0, x_parts[0].T, precision=highest)
        combined = combined + jnp.dot(w_parts[0], x_parts[1].T, precision=highest) / 256.0
        return combined * col_scale[:, None]
    combined = lax.map(column_block, blocks)
    product = combined.reshape(COLS, ROWS) * row_scale[None, :] / 16384.0
    mean_square = lax.optimization_barrier(jnp.mean(product * product, axis=0))
    normalized = product * lax.rsqrt(mean_square + epsilon)[None, :]
    return (row_scale, product, normalized)
```

```python
import functools

import jax
import jax.numpy as jnp
from jax import lax
from jax.experimental import pallas as pl
from jax.experimental.pallas import tpu as pltpu
from jax.sharding import PartitionSpec as P

epsilon = 1e-06
MESH = pl.DeviceIdType.MESH


def partner(me, step, count):
    if count & (count - 1):
        return lax.rem(step - me + count, count)
    out, bit = 0, 1
    while bit < count:
        out = out + bit * lax.rem(lax.div(me, bit) + lax.div(step, bit), 2)
        bit *= 2
    return out


def kernel(n_mp, n_rows, x_hbm, w_hbm, scale_out, product_out, norm_out,
           wq, wv, xv, sbuf, wbuf, xparts, xmax, psend, pbuf, gbuf, ssq, cscale,
           load_sem, z_send, z_recv, a_send, a_recv, b_send, b_recv,
           m_send, m_recv, p_send, p_recv, g_send, g_recv, q_send, q_recv):
    me, row = lax.axis_index("mp"), lax.axis_index("rows")
    n_b = 2 if n_rows % 2 == 0 else 1
    n_a = n_rows // n_b
    a, b = lax.div(row, n_b), lax.rem(row, n_b)
    total = n_mp * n_rows
    here = me * n_rows + row
    cols, inner_all = wv.shape
    rows, inner = xv.shape
    quarter = cols // n_rows

    def load(src, dst, at):
        return pltpu.make_async_copy(src, dst, load_sem.at[at])

    load_q = load(w_hbm.at[pl.ds(pl.multiple_of(row * quarter, quarter), quarter)], wq, 0)
    load_x = load(x_hbm, xv, 1)
    load_w = load(w_hbm, wv, 2)
    load_q.start()
    load_x.start()
    load_w.start()

    barrier = pltpu.get_barrier_semaphore()

    def greet(i, carry):
        to = lax.rem(here + i, total)
        pl.semaphore_signal(barrier, inc=1,
                            device_id={"mp": lax.div(to, n_rows), "rows": lax.rem(to, n_rows)},
                            device_id_type=MESH)
        return carry

    lax.fori_loop(1, total, greet, 0)

    load_q.wait()

    def block(i):
        return pl.ds(pl.multiple_of(i * inner, inner), inner)

    def widest(i, top):
        return jnp.maximum(top, jnp.max(jnp.abs(wq[:, block(i)]), axis=1, keepdims=True))

    top = lax.fori_loop(0, n_mp, widest, jnp.zeros((quarter, 1), jnp.float32)) + epsilon

    def cut(i, carry):
        t = wq[:, block(i)] / top * 128.0
        first = jnp.floor(t)
        sbuf[i, 0] = first.astype(jnp.bfloat16)
        sbuf[i, 1] = jnp.floor((t - first) * 256.0).astype(jnp.bfloat16)
        return carry

    lax.fori_loop(0, n_mp, cut, 0)

    def piece(who, at):
        return wbuf.at[who, :, pl.ds(pl.multiple_of(at * quarter, quarter), quarter), :]

    wbuf[me, :, pl.ds(pl.multiple_of(row * quarter, quarter), quarter), :] = sbuf[me]

    pl.semaphore_wait(barrier, total - 1)

    def remote(src, dst, send, recv, **where):
        return pltpu.make_async_remote_copy(src_ref=src, dst_ref=dst, send_sem=send, recv_sem=recv,
                                            device_id=where, device_id_type=MESH)

    def send_block(i, carry):
        to = partner(me, i, n_mp)

        @pl.when(to != me)
        def _():
            remote(sbuf.at[to], piece(me, row), z_send, z_recv.at[me], mp=to).start()
        return carry

    steps = lambda: (1, n_mp) if not (n_mp & (n_mp - 1)) else (0, n_mp)
    lax.fori_loop(*steps(), send_block, 0)

    def peer_a(k):
        return lax.rem(a + k, n_a) * n_b + b

    def peer_b(k):
        return a * n_b + lax.rem(b + k, n_b)

    def spread(who):
        for k in range(1, n_a):
            remote(piece(who, row), piece(who, row), a_send.at[k - 1],
                   a_recv.at[k - 1, who], rows=peer_a(k)).start()
        for k in range(1, n_b):
            remote(piece(who, row), piece(who, row), b_send.at[(k - 1) * n_a],
                   b_recv.at[(k - 1) * n_a, who], rows=peer_b(k)).start()

    spread(me)

    load_x.wait()
    lanes = 128
    peak = jnp.zeros((rows, lanes), jnp.float32)
    for j in range(inner // lanes):
        peak = jnp.maximum(peak, jnp.abs(xv[:, j * lanes:(j + 1) * lanes]))
    xmax[me] = jnp.max(peak.T, axis=0, keepdims=True)

    def tell(i, carry):
        to = lax.rem(me + i, n_mp)
        remote(xmax.at[me], xmax.at[me], m_send, m_recv, mp=to).start()
        return carry

    lax.fori_loop(1, n_mp, tell, 0)

    load_w.wait()
    big = jnp.zeros((cols, lanes), jnp.float32)

    def widest_all(i, big):
        at = pl.multiple_of(i * inner, inner)
        for j in range(inner // lanes):
            big = jnp.maximum(big, jnp.abs(wv[:, pl.ds(at + j * lanes, lanes)]))
        return big

    big = lax.fori_loop(0, n_mp, widest_all, big)
    cscale[...] = jnp.broadcast_to(jnp.max(big, axis=1, keepdims=True) + epsilon, (cols, lanes))

    def slices_of_x():
        remote(xmax.at[pl.ds(0, n_mp - 1)], xmax.at[pl.ds(0, n_mp - 1)], m_send, m_recv, mp=me).wait_recv()
        row_scale = jnp.max(xmax[...], axis=0) + epsilon
        scale_out[...] = row_scale
        tall = jnp.broadcast_to(row_scale, (lanes, rows)).T
        for j in range(inner // lanes):
            at = slice(j * lanes, (j + 1) * lanes)
            t = xv[:, at] / tall * 128.0
            first = jnp.floor(t)
            xparts[0, :, at] = first.astype(jnp.bfloat16)
            xparts[1, :, at] = jnp.floor((t - first) * 256.0).astype(jnp.bfloat16)

    def dot(w_side, x_side):
        return lax.dot_general(w_side, x_side, (((1,), (1,)), ((), ())),
                               preferred_element_type=jnp.float32)

    def stage(i, carry):
        @pl.when(i < n_mp)
        def _():
            who = partner(me, i, n_mp) if not (n_mp & (n_mp - 1)) else lax.rem(me + i, n_mp)

            @pl.when(i > 0)
            def _():
                remote(piece(who, row), piece(who, row), z_send, z_recv.at[who], mp=me).wait_recv()
                spread(who)

        @pl.when((i >= 1) & (i < n_mp + 1))
        def _():
            who = partner(me, i - 1, n_mp) if not (n_mp & (n_mp - 1)) else lax.rem(me + i - 1, n_mp)
            for k in range(1, n_a):
                got = piece(who, lax.rem(a - k + n_a, n_a) * n_b + b)
                remote(got, got, a_send.at[k - 1], a_recv.at[k - 1, who], mp=me).wait_recv()
                for kb in range(1, n_b):
                    at = (kb - 1) * n_a + k
                    remote(got, got, b_send.at[at], b_recv.at[at, who], rows=peer_b(kb)).start()

        @pl.when(i == 2)
        def _():
            slices_of_x()

        @pl.when(i >= 2)
        def _():
            who = partner(me, i - 2, n_mp) if not (n_mp & (n_mp - 1)) else lax.rem(me + i - 2, n_mp)
            for kb in range(1, n_b):
                other_b = lax.rem(b - kb + n_b, n_b)
                for k in range(n_a):
                    at = (kb - 1) * n_a + k
                    got = piece(who, lax.rem(a - k + n_a, n_a) * n_b + other_b)
                    remote(got, got, b_send.at[at], b_recv.at[at, who], mp=me).wait_recv()
            pair = dot(wbuf[who].reshape(2 * cols, inner), xparts[0])
            cross = dot(wbuf[who, 0], xparts[1])
            psend[who] = pair[:cols] + (pair[cols:] + cross) / 256.0

            @pl.when(who != me)
            def _():
                remote(psend.at[who], pbuf.at[me], p_send, p_recv, mp=who).start()

            @pl.when(who == me)
            def _():
                pbuf[me] = psend[me]
        return carry

    lax.fori_loop(0, n_mp + 2, stage, 0)

    remote(pbuf.at[pl.ds(0, n_mp - 1)], pbuf.at[pl.ds(0, n_mp - 1)], p_send, p_recv, mp=me).wait_recv()
    summed = lax.fori_loop(0, n_mp, lambda i, acc: acc + pbuf[i], jnp.zeros((cols, rows), jnp.float32))
    product = summed * cscale[:, :1] * scale_out[...] / float(inner_all)
    gbuf[row] = product
    ssq[here] = jnp.sum(product * product, axis=0, keepdims=True)

    for k in range(1, n_rows):
        remote(gbuf.at[row], gbuf.at[row], g_send, g_recv.at[k - 1], rows=lax.rem(row + k, n_rows)).start()

    def share(i, carry):
        to = lax.rem(here + i, total)
        remote(ssq.at[here], ssq.at[here], q_send, q_recv,
               mp=lax.div(to, n_rows), rows=lax.rem(to, n_rows)).start()
        return carry

    lax.fori_loop(1, total, share, 0)
    product_out[...] = product
    everyone = ssq.at[pl.ds(0, total - 1)]
    remote(everyone, everyone, q_send, q_recv, mp=me).wait_recv()

    for k in range(n_rows):
        src = lax.rem(row - k + n_rows, n_rows)
        if k:
            remote(gbuf.at[src], gbuf.at[src], g_send, g_recv.at[k - 1], mp=me).wait_recv()
        squares = lax.fori_loop(0, n_mp, lambda i, acc: acc + ssq[i * n_rows + src],
                                jnp.zeros((1, rows), jnp.float32))
        factor = lax.rsqrt(squares / float(cols * n_mp) + epsilon)
        norm_out[:, pl.ds(pl.multiple_of(src * rows, rows), rows)] = gbuf[src] * factor

    def left(ref, sem):
        remote(ref, ref, sem, q_recv, mp=me).wait_send()

    left(sbuf.at[pl.ds(0, n_mp - 1)], z_send)
    for k in range(n_a - 1):
        left(sbuf, a_send.at[k])
    for k in range(n_a * (n_b - 1)):
        left(sbuf, b_send.at[k])
    left(xmax.at[pl.ds(0, n_mp - 1)], m_send)
    left(psend.at[pl.ds(0, n_mp - 1)], p_send)
    left(gbuf.at[pl.ds(0, n_rows - 1)], g_send)
    left(everyone, q_send)


def per_device(n_mp, n_rows, inputs, weight):
    rows, inner = inputs.shape
    cols, inner_all = weight.shape
    quarter = cols // n_rows
    f32, bf16 = jnp.float32, jnp.bfloat16
    n_b = 2 if n_rows % 2 == 0 else 1
    n_a = n_rows // n_b
    dma = pltpu.SemaphoreType.DMA
    vmem = pl.BlockSpec(memory_space=pltpu.VMEM)
    scale, product, normalized = pl.pallas_call(
        functools.partial(kernel, n_mp, n_rows),
        out_shape=(jax.ShapeDtypeStruct((1, rows), f32),
                   jax.ShapeDtypeStruct((cols, rows), f32),
                   jax.ShapeDtypeStruct((cols, rows * n_rows), f32)),
        in_specs=[pl.BlockSpec(memory_space=pl.ANY)] * 2,
        out_specs=(vmem, vmem, vmem),
        scratch_shapes=[
            pltpu.VMEM((quarter, inner_all), f32),
            pltpu.VMEM((cols, inner_all), f32),
            pltpu.VMEM((rows, inner), f32),
            pltpu.VMEM((n_mp, 2, quarter, inner), bf16),
            pltpu.VMEM((n_mp, 2, cols, inner), bf16),
            pltpu.VMEM((2, rows, inner), bf16),
            pltpu.VMEM((n_mp, 1, rows), f32),
            pltpu.VMEM((n_mp, cols, rows), f32),
            pltpu.VMEM((n_mp, cols, rows), f32),
            pltpu.VMEM((n_rows, cols, rows), f32),
            pltpu.VMEM((n_mp * n_rows, 1, rows), f32),
            pltpu.VMEM((cols, 128), f32),
            dma((3,)), dma, dma((n_mp,)),
            dma((max(n_a - 1, 1),)), dma((max(n_a - 1, 1), n_mp)),
            dma((max(n_a * (n_b - 1), 1),)), dma((max(n_a * (n_b - 1), 1), n_mp)),
            dma, dma, dma, dma, dma, dma((max(n_rows - 1, 1),)), dma, dma,
        ],
        compiler_params=pltpu.CompilerParams(
            collective_id=0, has_side_effects=True, vmem_limit_bytes=60 * 2**20
        ),
        name="split_product",
    )(inputs, weight)
    return scale.reshape(rows), product, normalized


def solution(mesh):
    return jax.shard_map(
        functools.partial(per_device, mesh.shape["mp"], mesh.shape["rows"]),
        mesh=mesh,
        in_specs=(P("rows", "mp"), P("mp", None)),
        out_specs=(P("rows"), P("mp", "rows"), P("mp", None)),
        check_vma=False,
    )
```

```python
import functools

import jax
import jax.numpy as jnp
from jax import lax
from jax.experimental import pallas as pl
from jax.experimental.pallas import tpu as pltpu
from jax.sharding import PartitionSpec as P

epsilon = 1e-06
MESH = pl.DeviceIdType.MESH


def partner(me, step, count):
    if count & (count - 1):
        return lax.rem(step - me + count, count)
    out, bit = 0, 1
    while bit < count:
        out = out + bit * lax.rem(lax.div(me, bit) + lax.div(step, bit), 2)
        bit *= 2
    return out


def kernel(n_mp, n_rows, x_hbm, w_hbm, scale_out, product_out, norm_out,
           wv, xv, sbuf, wbuf, xparts, xmax, psend, pbuf, gbuf, ssq, cscale,
           load_sem, z_send, z_recv, a_send, a_recv, b_send, b_recv,
           m_send, m_recv, p_send, p_recv, g_send, g_recv, q_send, q_recv):
    me, row = lax.axis_index("mp"), lax.axis_index("rows")
    n_b = 2 if n_rows % 2 == 0 else 1
    n_a = n_rows // n_b
    a, b = lax.div(row, n_b), lax.rem(row, n_b)
    total = n_mp * n_rows
    here = me * n_rows + row
    cols, inner_all = wv.shape
    rows, inner = xv.shape
    quarter = cols // n_rows

    half = cols // n_b
    share_at = b * n_a + a
    even = not (n_mp & (n_mp - 1)) and n_mp >= 4
    near = n_mp // 2 if even else n_mp
    fourth = n_mp // 4
    middle = lax.rem(lax.div(me + fourth, near), 2) if even else 0

    def load(at, index):
        rows_at = pl.ds(pl.multiple_of(at * half, half), half)
        return pltpu.make_async_copy(w_hbm.at[rows_at], wv.at[rows_at], load_sem.at[index])

    loads = [load(lax.rem(b + k, n_b), 1 + k) for k in range(n_b)]
    load_x = pltpu.make_async_copy(x_hbm, xv, load_sem.at[0])
    loads[0].start()
    load_x.start()
    for other in loads[1:]:
        other.start()

    barrier = pltpu.get_barrier_semaphore()

    def greet(i, carry):
        to = lax.rem(here + i, total)
        pl.semaphore_signal(barrier, inc=1,
                            device_id={"mp": lax.div(to, n_rows), "rows": lax.rem(to, n_rows)},
                            device_id_type=MESH)
        return carry

    lax.fori_loop(1, total, greet, 0)

    def other_mp(step):
        return partner(me, step, n_mp) if even else lax.rem(me + step, n_mp)

    lanes = 128

    def scale_of(at, count):
        def widest(i, big):
            first = pl.multiple_of(i * inner, inner)
            for j in range(inner // lanes):
                big = jnp.maximum(big, jnp.abs(wv[pl.ds(at, count), pl.ds(first + j * lanes, lanes)]))
            return big

        big = lax.fori_loop(0, n_mp, widest, jnp.zeros((count, lanes), jnp.float32))
        cscale[pl.ds(at, count)] = jnp.broadcast_to(
            jnp.max(big, axis=1, keepdims=True) + epsilon, (count, lanes))

    def cut(at, count, block):
        inverse = 128.0 / cscale[pl.ds(at, count), :1]
        t = wv[pl.ds(at, count), pl.ds(pl.multiple_of(block * inner, inner), inner)] * inverse
        first = jnp.floor(t)
        return first.astype(jnp.bfloat16), jnp.floor((t - first) * 256.0).astype(jnp.bfloat16)

    loads[0].wait()
    half_at = pl.multiple_of(b * half, half)
    quarter_at = pl.multiple_of(share_at * quarter, quarter)
    scale_of(half_at, half)

    def piece(who, at):
        return wbuf.at[who, :, pl.ds(pl.multiple_of(at * quarter, quarter), quarter), :]

    def wide_piece(who, at):
        return wbuf.at[who, :, pl.ds(pl.multiple_of(at * half, half), half), :]

    def remote(src, dst, send, recv, **where):
        return pltpu.make_async_remote_copy(src_ref=src, dst_ref=dst, send_sem=send, recv_sem=recv,
                                            device_id=where, device_id_type=MESH)

    pl.semaphore_wait(barrier, total - 1)

    def send_block(i, carry):
        step = lax.rem(i + middle * near, n_mp)
        to = other_mp(step)

        @pl.when((step > 0) & (step < near))
        def _():
            first, second = cut(half_at, half, to)
            sbuf[to, 0] = first
            sbuf[to, 1] = second
            remote(sbuf.at[to], wide_piece(me, b), z_send.at[0], z_recv.at[me], mp=to).start()

        @pl.when(step >= near)
        def _():
            first, second = cut(quarter_at, quarter, to)
            sbuf[to, 0, :quarter] = first
            sbuf[to, 1, :quarter] = second
            remote(sbuf.at[to, :, pl.ds(0, quarter), :], piece(me, share_at), z_send.at[1],
                   z_recv.at[me], mp=to).start()
        return carry

    lax.fori_loop(0, n_mp, send_block, 0)

    def peer_a(k):
        return lax.rem(a + k, n_a) * n_b + b

    def peer_b(k):
        return a * n_b + lax.rem(b + k, n_b)

    def from_mp(i):
        if not even:
            return i, lax.rem(me - i + n_mp, n_mp)
        group, rest = lax.div(i, fourth), lax.rem(i, fourth)
        odd, high = lax.rem(group, 2), lax.div(group, 2)
        step = (odd * 2 + high + middle * odd * (1 - 2 * high)) * fourth + rest
        return step, other_mp(step)

    load_x.wait()
    peak = jnp.zeros((rows, lanes), jnp.float32)
    for j in range(inner // lanes):
        peak = jnp.maximum(peak, jnp.abs(xv[:, j * lanes:(j + 1) * lanes]))
    xmax[me] = jnp.max(peak.T, axis=0, keepdims=True)

    def tell(i, carry):
        to = lax.rem(me + i, n_mp)
        remote(xmax.at[me], xmax.at[me], m_send, m_recv, mp=to).start()
        return carry

    lax.fori_loop(1, n_mp, tell, 0)

    for k in range(1, n_b):
        loads[k].wait()
        scale_of(pl.multiple_of(lax.rem(b + k, n_b) * half, half), half)
    for k in range(n_b):
        first, second = cut(k * half, half, me)
        wbuf[me, 0, k * half:(k + 1) * half] = first
        wbuf[me, 1, k * half:(k + 1) * half] = second

    def slices_of_x():
        remote(xmax.at[pl.ds(0, n_mp - 1)], xmax.at[pl.ds(0, n_mp - 1)], m_send, m_recv, mp=me).wait_recv()
        row_scale = jnp.max(xmax[...], axis=0) + epsilon
        scale_out[...] = row_scale
        tall = jnp.broadcast_to(128.0 / row_scale, (lanes, rows)).T
        for j in range(inner // lanes):
            at = slice(j * lanes, (j + 1) * lanes)
            t = xv[:, at] * tall
            first = jnp.floor(t)
            xparts[0, :, at] = first.astype(jnp.bfloat16)
            xparts[1, :, at] = jnp.floor((t - first) * 256.0).astype(jnp.bfloat16)

    def dot(w_side, x_side):
        return lax.dot_general(w_side, x_side, (((1,), (1,)), ((), ())),
                               preferred_element_type=jnp.float32)

    wide_at = n_a * (n_b - 1)

    def stage(i, carry):
        @pl.when(i < n_mp)
        def _():
            step, who = from_mp(i)

            @pl.when((step > 0) & (step < near))
            def _():
                got = wide_piece(who, b)
                remote(got, got, z_send.at[0], z_recv.at[who], mp=me).wait_recv()
                for kb in range(1, n_b):
                    remote(got, got, b_send.at[wide_at + kb - 1], b_recv.at[(kb - 1) * n_a, who],
                           rows=peer_b(kb)).start()

            @pl.when(step >= near)
            def _():
                got = piece(who, share_at)
                remote(got, got, z_send.at[1], z_recv.at[who], mp=me).wait_recv()
                for k in range(1, n_a):
                    remote(got, got, a_send.at[k - 1], a_recv.at[k - 1, who], rows=peer_a(k)).start()
                for kb in range(1, n_b):
                    remote(got, got, b_send.at[(kb - 1) * n_a], b_recv.at[(kb - 1) * n_a, who],
                           rows=peer_b(kb)).start()

        @pl.when((i >= 1) & (i < n_mp + 1))
        def _():
            step, who = from_mp(i - 1)

            @pl.when(step >= near)
            def _():
                for k in range(1, n_a):
                    got = piece(who, b * n_a + lax.rem(a - k + n_a, n_a))
                    remote(got, got, a_send.at[k - 1], a_recv.at[k - 1, who], mp=me).wait_recv()
                    for kb in range(1, n_b):
                        at = (kb - 1) * n_a + k
                        remote(got, got, b_send.at[at], b_recv.at[at, who], rows=peer_b(kb)).start()

        @pl.when(i == 2)
        def _():
            slices_of_x()

        @pl.when(i >= 2)
        def _():
            step, who = from_mp(i - 2)

            @pl.when((step > 0) & (step < near))
            def _():
                for kb in range(1, n_b):
                    got = wide_piece(who, lax.rem(b - kb + n_b, n_b))
                    remote(got, got, b_send.at[wide_at + kb - 1], b_recv.at[(kb - 1) * n_a, who],
                           mp=me).wait_recv()

            @pl.when(step >= near)
            def _():
                for kb in range(1, n_b):
                    other_b = lax.rem(b - kb + n_b, n_b)
                    for k in range(n_a):
                        at = (kb - 1) * n_a + k
                        got = piece(who, other_b * n_a + lax.rem(a - k + n_a, n_a))
                        remote(got, got, b_send.at[at], b_recv.at[at, who], mp=me).wait_recv()
            pair = dot(wbuf[who].reshape(2 * cols, inner), xparts[0])
            cross = dot(wbuf[who, 0], xparts[1])
            psend[who] = pair[:cols] + (pair[cols:] + cross) / 256.0

            @pl.when(who != me)
            def _():
                remote(psend.at[who], pbuf.at[me], p_send, p_recv, mp=who).start()

            @pl.when(who == me)
            def _():
                pbuf[me] = psend[me]
        return carry

    lax.fori_loop(0, n_mp + 2, stage, 0)

    remote(pbuf.at[pl.ds(0, n_mp - 1)], pbuf.at[pl.ds(0, n_mp - 1)], p_send, p_recv, mp=me).wait_recv()
    summed = lax.fori_loop(0, n_mp, lambda i, acc: acc + pbuf[i], jnp.zeros((cols, rows), jnp.float32))
    product = summed * cscale[:, :1] * scale_out[...] / float(inner_all)
    gbuf[row] = product
    ssq[here] = jnp.sum(product * product, axis=0, keepdims=True)

    for k in range(1, n_rows):
        remote(gbuf.at[row], gbuf.at[row], g_send, g_recv.at[k - 1], rows=lax.rem(row + k, n_rows)).start()

    def share(i, carry):
        to = lax.rem(here + i, total)
        remote(ssq.at[here], ssq.at[here], q_send, q_recv,
               mp=lax.div(to, n_rows), rows=lax.rem(to, n_rows)).start()
        return carry

    lax.fori_loop(1, total, share, 0)
    product_out[...] = product
    everyone = ssq.at[pl.ds(0, total - 1)]
    remote(everyone, everyone, q_send, q_recv, mp=me).wait_recv()

    for k in range(n_rows):
        src = lax.rem(row - k + n_rows, n_rows)
        if k:
            remote(gbuf.at[src], gbuf.at[src], g_send, g_recv.at[k - 1], mp=me).wait_recv()
        squares = lax.fori_loop(0, n_mp, lambda i, acc: acc + ssq[i * n_rows + src],
                                jnp.zeros((1, rows), jnp.float32))
        factor = lax.rsqrt(squares / float(cols * n_mp) + epsilon)
        norm_out[:, pl.ds(pl.multiple_of(src * rows, rows), rows)] = gbuf[src] * factor

    def left(ref, sem):
        remote(ref, ref, sem, q_recv, mp=me).wait_send()

    left(sbuf.at[pl.ds(0, near - 1)], z_send.at[0])
    for kb in range(n_b - 1):
        left(sbuf.at[pl.ds(0, near - 1)], b_send.at[wide_at + kb])
    if near < n_mp:
        narrow = sbuf.at[pl.ds(0, n_mp - near), :, pl.ds(0, quarter), :]
        left(narrow, z_send.at[1])
        for k in range(n_a - 1):
            left(narrow, a_send.at[k])
        for k in range(n_a * (n_b - 1)):
            left(narrow, b_send.at[k])
    left(xmax.at[pl.ds(0, n_mp - 1)], m_send)
    left(psend.at[pl.ds(0, n_mp - 1)], p_send)
    left(gbuf.at[pl.ds(0, n_rows - 1)], g_send)
    left(everyone, q_send)


def hand_over(scale, product, normalized, scale_out, product_out, norm_out):
    scale_out[...] = scale[...]
    product_out[...] = product[...]
    norm_out[...] = normalized[...]


def per_device(n_mp, n_rows, inputs, weight):
    rows, inner = inputs.shape
    cols, inner_all = weight.shape
    quarter = cols // n_rows
    f32, bf16 = jnp.float32, jnp.bfloat16
    n_b = 2 if n_rows % 2 == 0 else 1
    n_a = n_rows // n_b
    dma = pltpu.SemaphoreType.DMA
    vmem = pl.BlockSpec(memory_space=pltpu.VMEM)
    scale, product, normalized = pl.pallas_call(
        functools.partial(kernel, n_mp, n_rows),
        out_shape=(jax.ShapeDtypeStruct((1, rows), f32),
                   jax.ShapeDtypeStruct((cols, rows), f32),
                   jax.ShapeDtypeStruct((cols, rows * n_rows), f32)),
        in_specs=[pl.BlockSpec(memory_space=pl.ANY)] * 2,
        out_specs=(vmem, vmem, vmem),
        scratch_shapes=[
            pltpu.VMEM((cols, inner_all), f32),
            pltpu.VMEM((rows, inner), f32),
            pltpu.VMEM((n_mp, 2, cols // n_b, inner), bf16),
            pltpu.VMEM((n_mp, 2, cols, inner), bf16),
            pltpu.VMEM((2, rows, inner), bf16),
            pltpu.VMEM((n_mp, 1, rows), f32),
            pltpu.VMEM((n_mp, cols, rows), f32),
            pltpu.VMEM((n_mp, cols, rows), f32),
            pltpu.VMEM((n_rows, cols, rows), f32),
            pltpu.VMEM((n_mp * n_rows, 1, rows), f32),
            pltpu.VMEM((cols, 128), f32),
            dma((1 + n_b,)), dma((2,)), dma((n_mp,)),
            dma((max(n_a - 1, 1),)), dma((max(n_a - 1, 1), n_mp)),
            dma((max((n_a + 1) * (n_b - 1), 1),)), dma((max(n_a * (n_b - 1), 1), n_mp)),
            dma, dma, dma, dma, dma, dma((max(n_rows - 1, 1),)), dma, dma,
        ],
        compiler_params=pltpu.CompilerParams(
            collective_id=0, has_side_effects=True, vmem_limit_bytes=60 * 2**20
        ),
        name="split_product",
    )(inputs, weight)
    scale, product, normalized = pl.pallas_call(
        hand_over,
        out_shape=tuple(jax.ShapeDtypeStruct(each.shape, f32) for each in (scale, product, normalized)),
        in_specs=[vmem] * 3,
        out_specs=(vmem, vmem, vmem),
        name="hand_over",
    )(scale, product, normalized)
    return scale.reshape(rows), product, normalized


def solution(mesh):
    return jax.shard_map(
        functools.partial(per_device, mesh.shape["mp"], mesh.shape["rows"]),
        mesh=mesh,
        in_specs=(P("rows", "mp"), P("mp", None)),
        out_specs=(P("rows"), P("mp", "rows"), P("mp", None)),
        check_vma=False,
    )
```

```python
import functools

import jax
import jax.numpy as jnp
from jax import lax
from jax.experimental import pallas as pl
from jax.experimental.pallas import tpu as pltpu
from jax.sharding import PartitionSpec as P

epsilon = 1e-06
MESH = pl.DeviceIdType.MESH


def partner(me, step, count):
    if count & (count - 1):
        return lax.rem(step - me + count, count)
    out, bit = 0, 1
    while bit < count:
        out = out + bit * lax.rem(lax.div(me, bit) + lax.div(step, bit), 2)
        bit *= 2
    return out


def kernel(n_mp, n_rows, x_hbm, w_hbm, scale_out, product_out, norm_out,
           wq, wv, xv, sbuf, wbuf, xparts, xmax, psend, pbuf, gbuf, ssq, cscale,
           load_sem, z_send, z_recv, a_send, a_recv, b_send, b_recv,
           m_send, m_recv, p_send, p_recv, g_send, g_recv, q_send, q_recv):
    me, row = lax.axis_index("mp"), lax.axis_index("rows")
    n_b = 2 if n_rows % 2 == 0 else 1
    n_a = n_rows // n_b
    a, b = lax.div(row, n_b), lax.rem(row, n_b)
    total = n_mp * n_rows
    here = me * n_rows + row
    cols, inner_all = wv.shape
    rows, inner = xv.shape
    quarter = cols // n_rows

    def load(src, dst, at):
        return pltpu.make_async_copy(src, dst, load_sem.at[at])

    load_q = load(w_hbm.at[pl.ds(pl.multiple_of(row * quarter, quarter), quarter)], wq, 0)
    load_x = load(x_hbm, xv, 1)
    load_w = load(w_hbm, wv, 2)
    load_q.start()
    load_x.start()
    load_w.start()

    barrier = pltpu.get_barrier_semaphore()

    def greet(i, carry):
        to = lax.rem(here + i, total)
        pl.semaphore_signal(barrier, inc=1,
                            device_id={"mp": lax.div(to, n_rows), "rows": lax.rem(to, n_rows)},
                            device_id_type=MESH)
        return carry

    lax.fori_loop(1, total, greet, 0)

    load_q.wait()

    def block(i):
        return pl.ds(pl.multiple_of(i * inner, inner), inner)

    def widest(i, top):
        return jnp.maximum(top, jnp.max(jnp.abs(wq[:, block(i)]), axis=1, keepdims=True))

    top = lax.fori_loop(0, n_mp, widest, jnp.zeros((quarter, 1), jnp.float32)) + epsilon

    def cut(i, carry):
        t = wq[:, block(i)] / top * 128.0
        first = jnp.floor(t)
        sbuf[i, 0] = first.astype(jnp.bfloat16)
        sbuf[i, 1] = jnp.floor((t - first) * 256.0).astype(jnp.bfloat16)
        return carry

    lax.fori_loop(0, n_mp, cut, 0)

    def piece(who, at):
        return wbuf.at[who, :, pl.ds(pl.multiple_of(at * quarter, quarter), quarter), :]

    wbuf[me, :, pl.ds(pl.multiple_of(row * quarter, quarter), quarter), :] = sbuf[me]

    pl.semaphore_wait(barrier, total - 1)

    def remote(src, dst, send, recv, **where):
        return pltpu.make_async_remote_copy(src_ref=src, dst_ref=dst, send_sem=send, recv_sem=recv,
                                            device_id=where, device_id_type=MESH)

    def send_block(i, carry):
        to = partner(me, i, n_mp)

        @pl.when(to != me)
        def _():
            remote(sbuf.at[to], piece(me, row), z_send, z_recv.at[me], mp=to).start()
        return carry

    steps = lambda: (1, n_mp) if not (n_mp & (n_mp - 1)) else (0, n_mp)
    lax.fori_loop(*steps(), send_block, 0)

    def peer_a(k):
        return lax.rem(a + k, n_a) * n_b + b

    def peer_b(k):
        return a * n_b + lax.rem(b + k, n_b)

    def spread(who):
        for k in range(1, n_a):
            remote(piece(who, row), piece(who, row), a_send.at[k - 1],
                   a_recv.at[k - 1, who], rows=peer_a(k)).start()
        for k in range(1, n_b):
            remote(piece(who, row), piece(who, row), b_send.at[(k - 1) * n_a],
                   b_recv.at[(k - 1) * n_a, who], rows=peer_b(k)).start()

    spread(me)

    load_x.wait()
    lanes = 128
    peak = jnp.zeros((rows, lanes), jnp.float32)
    for j in range(inner // lanes):
        peak = jnp.maximum(peak, jnp.abs(xv[:, j * lanes:(j + 1) * lanes]))
    xmax[me] = jnp.max(peak.T, axis=0, keepdims=True)

    def tell(i, carry):
        to = lax.rem(me + i, n_mp)
        remote(xmax.at[me], xmax.at[me], m_send, m_recv, mp=to).start()
        return carry

    lax.fori_loop(1, n_mp, tell, 0)

    load_w.wait()
    big = jnp.zeros((cols, lanes), jnp.float32)

    def widest_all(i, big):
        at = pl.multiple_of(i * inner, inner)
        for j in range(inner // lanes):
            big = jnp.maximum(big, jnp.abs(wv[:, pl.ds(at + j * lanes, lanes)]))
        return big

    big = lax.fori_loop(0, n_mp, widest_all, big)
    cscale[...] = jnp.broadcast_to(jnp.max(big, axis=1, keepdims=True) + epsilon, (cols, lanes))

    def slices_of_x():
        remote(xmax.at[pl.ds(0, n_mp - 1)], xmax.at[pl.ds(0, n_mp - 1)], m_send, m_recv, mp=me).wait_recv()
        row_scale = jnp.max(xmax[...], axis=0) + epsilon
        scale_out[...] = row_scale
        tall = jnp.broadcast_to(row_scale, (lanes, rows)).T
        for j in range(inner // lanes):
            at = slice(j * lanes, (j + 1) * lanes)
            t = xv[:, at] / tall * 128.0
            first = jnp.floor(t)
            xparts[0, :, at] = first.astype(jnp.bfloat16)
            xparts[1, :, at] = jnp.floor((t - first) * 256.0).astype(jnp.bfloat16)

    def dot(w_side, x_side):
        return lax.dot_general(w_side, x_side, (((1,), (1,)), ((), ())),
                               preferred_element_type=jnp.float32)

    def stage(i, carry):
        @pl.when(i < n_mp)
        def _():
            who = partner(me, i, n_mp) if not (n_mp & (n_mp - 1)) else lax.rem(me + i, n_mp)

            @pl.when(i > 0)
            def _():
                remote(piece(who, row), piece(who, row), z_send, z_recv.at[who], mp=me).wait_recv()
                spread(who)

        @pl.when((i >= 1) & (i < n_mp + 1))
        def _():
            who = partner(me, i - 1, n_mp) if not (n_mp & (n_mp - 1)) else lax.rem(me + i - 1, n_mp)
            for k in range(1, n_a):
                got = piece(who, lax.rem(a - k + n_a, n_a) * n_b + b)
                remote(got, got, a_send.at[k - 1], a_recv.at[k - 1, who], mp=me).wait_recv()
                for kb in range(1, n_b):
                    at = (kb - 1) * n_a + k
                    remote(got, got, b_send.at[at], b_recv.at[at, who], rows=peer_b(kb)).start()

        @pl.when(i == 2)
        def _():
            slices_of_x()

        @pl.when(i >= 2)
        def _():
            who = partner(me, i - 2, n_mp) if not (n_mp & (n_mp - 1)) else lax.rem(me + i - 2, n_mp)
            for kb in range(1, n_b):
                other_b = lax.rem(b - kb + n_b, n_b)
                for k in range(n_a):
                    at = (kb - 1) * n_a + k
                    got = piece(who, lax.rem(a - k + n_a, n_a) * n_b + other_b)
                    remote(got, got, b_send.at[at], b_recv.at[at, who], mp=me).wait_recv()
            pair = dot(wbuf[who].reshape(2 * cols, inner), xparts[0])
            cross = dot(wbuf[who, 0], xparts[1])
            psend[who] = pair[:cols] + (pair[cols:] + cross) / 256.0

            @pl.when(who != me)
            def _():
                remote(psend.at[who], pbuf.at[me], p_send, p_recv, mp=who).start()

            @pl.when(who == me)
            def _():
                pbuf[me] = psend[me]
        return carry

    lax.fori_loop(0, n_mp + 2, stage, 0)

    remote(pbuf.at[pl.ds(0, n_mp - 1)], pbuf.at[pl.ds(0, n_mp - 1)], p_send, p_recv, mp=me).wait_recv()
    summed = lax.fori_loop(0, n_mp, lambda i, acc: acc + pbuf[i], jnp.zeros((cols, rows), jnp.float32))
    product = summed * cscale[:, :1] * scale_out[...] / float(inner_all)
    gbuf[row] = product
    ssq[here] = jnp.sum(product * product, axis=0, keepdims=True)

    for k in range(1, n_rows):
        remote(gbuf.at[row], gbuf.at[row], g_send, g_recv.at[k - 1], rows=lax.rem(row + k, n_rows)).start()

    def share(i, carry):
        to = lax.rem(here + i, total)
        remote(ssq.at[here], ssq.at[here], q_send, q_recv,
               mp=lax.div(to, n_rows), rows=lax.rem(to, n_rows)).start()
        return carry

    lax.fori_loop(1, total, share, 0)
    product_out[...] = product
    everyone = ssq.at[pl.ds(0, total - 1)]
    remote(everyone, everyone, q_send, q_recv, mp=me).wait_recv()

    for k in range(n_rows):
        src = lax.rem(row - k + n_rows, n_rows)
        if k:
            remote(gbuf.at[src], gbuf.at[src], g_send, g_recv.at[k - 1], mp=me).wait_recv()
        squares = lax.fori_loop(0, n_mp, lambda i, acc: acc + ssq[i * n_rows + src],
                                jnp.zeros((1, rows), jnp.float32))
        factor = lax.rsqrt(squares / float(cols * n_mp) + epsilon)
        norm_out[:, pl.ds(pl.multiple_of(src * rows, rows), rows)] = gbuf[src] * factor

    def left(ref, sem):
        remote(ref, ref, sem, q_recv, mp=me).wait_send()

    left(sbuf.at[pl.ds(0, n_mp - 1)], z_send)
    for k in range(n_a - 1):
        left(sbuf, a_send.at[k])
    for k in range(n_a * (n_b - 1)):
        left(sbuf, b_send.at[k])
    left(xmax.at[pl.ds(0, n_mp - 1)], m_send)
    left(psend.at[pl.ds(0, n_mp - 1)], p_send)
    left(gbuf.at[pl.ds(0, n_rows - 1)], g_send)
    left(everyone, q_send)


def hand_over(scale, product, normalized, scale_out, product_out, norm_out):
    scale_out[...] = scale[...]
    product_out[...] = product[...]
    norm_out[...] = normalized[...]


def per_device(n_mp, n_rows, inputs, weight):
    rows, inner = inputs.shape
    cols, inner_all = weight.shape
    quarter = cols // n_rows
    f32, bf16 = jnp.float32, jnp.bfloat16
    n_b = 2 if n_rows % 2 == 0 else 1
    n_a = n_rows // n_b
    dma = pltpu.SemaphoreType.DMA
    vmem = pl.BlockSpec(memory_space=pltpu.VMEM)
    scale, product, normalized = pl.pallas_call(
        functools.partial(kernel, n_mp, n_rows),
        out_shape=(jax.ShapeDtypeStruct((1, rows), f32),
                   jax.ShapeDtypeStruct((cols, rows), f32),
                   jax.ShapeDtypeStruct((cols, rows * n_rows), f32)),
        in_specs=[pl.BlockSpec(memory_space=pl.ANY)] * 2,
        out_specs=(vmem, vmem, vmem),
        scratch_shapes=[
            pltpu.VMEM((quarter, inner_all), f32),
            pltpu.VMEM((cols, inner_all), f32),
            pltpu.VMEM((rows, inner), f32),
            pltpu.VMEM((n_mp, 2, quarter, inner), bf16),
            pltpu.VMEM((n_mp, 2, cols, inner), bf16),
            pltpu.VMEM((2, rows, inner), bf16),
            pltpu.VMEM((n_mp, 1, rows), f32),
            pltpu.VMEM((n_mp, cols, rows), f32),
            pltpu.VMEM((n_mp, cols, rows), f32),
            pltpu.VMEM((n_rows, cols, rows), f32),
            pltpu.VMEM((n_mp * n_rows, 1, rows), f32),
            pltpu.VMEM((cols, 128), f32),
            dma((3,)), dma, dma((n_mp,)),
            dma((max(n_a - 1, 1),)), dma((max(n_a - 1, 1), n_mp)),
            dma((max(n_a * (n_b - 1), 1),)), dma((max(n_a * (n_b - 1), 1), n_mp)),
            dma, dma, dma, dma, dma, dma((max(n_rows - 1, 1),)), dma, dma,
        ],
        compiler_params=pltpu.CompilerParams(
            collective_id=0, has_side_effects=True, vmem_limit_bytes=60 * 2**20
        ),
        name="split_product",
    )(inputs, weight)
    scale, product, normalized = pl.pallas_call(
        hand_over,
        out_shape=tuple(jax.ShapeDtypeStruct(each.shape, f32) for each in (scale, product, normalized)),
        in_specs=[vmem] * 3,
        out_specs=(vmem, vmem, vmem),
        name="hand_over",
    )(scale, product, normalized)
    return scale.reshape(rows), product, normalized


def solution(mesh):
    return jax.shard_map(
        functools.partial(per_device, mesh.shape["mp"], mesh.shape["rows"]),
        mesh=mesh,
        in_specs=(P("rows", "mp"), P("mp", None)),
        out_specs=(P("rows"), P("mp", "rows"), P("mp", None)),
        check_vma=False,
    )
```
